8 devices in a mesh: rep: 1 (over z), dp: 8 (over x, y, core).
Axes of the slice: x: 2, y: 2, z: 1, core: 2. Of those that a mesh axis runs over, the one named last changes fastest.
Arguments:
- x: bfloat16 [8, 2048, 512], P(('rep', 'dp'))
- dy: bfloat16 [8, 2048, 512], P(('rep', 'dp'))
- w_gate: bfloat16 [2, 512, 8192], replicated
- w_up: bfloat16 [2, 512, 8192], replicated
- w_down: bfloat16 [2, 8192, 512], replicated
- m_w_gate: float32 [2, 512, 8192], P(None, 'dp')
- m_w_up: float32 [2, 512, 8192], P(None, 'dp')
- m_w_down: float32 [2, 8192, 512], P(None, 'dp')
- v_w_gate: float32 [2, 512, 8192], P(None, 'dp')
- v_w_up: float32 [2, 512, 8192], P(None, 'dp')
- v_w_down: float32 [2, 8192, 512], P(None, 'dp')
Outputs:
- output 1: bfloat16 [2, 512, 8192], P('rep')
- output 2: bfloat16 [2, 512, 8192], P('rep')
- output 3: bfloat16 [2, 8192, 512], P('rep')
- output 4: float32 [2, 512, 8192], P('rep', 'dp')
- output 5: float32 [2, 512, 8192], P('rep', 'dp')
- output 6: float32 [2, 8192, 512], P('rep', 'dp')
- output 7: float32 [2, 512, 8192], P('rep', 'dp')
- output 8: float32 [2, 512, 8192], P('rep', 'dp')
- output 9: float32 [2, 8192, 512], P('rep', 'dp')
All inputs are finite; a program needn't handle non-finite values.
Results may differ from the reference program's by a relative error of at most 0.022.
Values are sent between devices in bfloat16 or wider.
A program may use at most 2 GiB of HBM per device.

```python
import jax
import jax.numpy as jnp
from jax import lax

SEQUENCES = 8
TOKENS = 2048
D = 512
FF = 8192
LAYERS = 2
NAMES = ("w_gate", "w_up", "w_down")
SHAPES = {"w_gate": (LAYERS, D, FF), "w_up": (LAYERS, D, FF), "w_down": (LAYERS, FF, D)}


def bump(key, n, height):
    away = (jnp.arange(n, dtype=jnp.int32) - jax.random.randint(key, (), 0, n, jnp.int32)) % n
    return jnp.where(away < n // 8, height, 1.0)


def together(key, own, strength):
    shared = jax.random.normal(key, own.shape[1:], jnp.float32)
    return (own + strength * shared) * lax.rsqrt(1 + strength * strength)


def setup_inputs(seed: int = 0, part: int = 0) -> dict:
    kx, kdy, ka, kb, kz, kf, kh, kl, *keys = jax.random.split(jax.random.key(seed), 8 + 3 * len(NAMES))
    kx, kdy, ka, kb = (jax.random.fold_in(k, part) for k in (kx, kdy, ka, kb))
    kw, km, kv = (keys[i::3] for i in range(3))
    shape = (SEQUENCES, TOKENS, D)
    much_x, much_dy = jax.random.uniform(kz, (2,), jnp.float32, 0.0, 1.0)
    loud = 2.0 ** jax.random.uniform(jax.random.fold_in(kz, 1), (), jnp.float32, -1.0, 2.0)
    layers = 2.0 ** jax.random.uniform(kl, (LAYERS, 1, 1), jnp.float32, -1.0, 1.0)
    x = together(ka, jax.random.normal(kx, shape, jnp.float32), much_x) * bump(kf, D, 4.0)
    dy = together(kb, jax.random.normal(kdy, shape, jnp.float32), much_dy)
    drawn = {"x": x.astype(jnp.bfloat16), "dy": (loud * dy * (SEQUENCES * TOKENS) ** -0.5).astype(jnp.bfloat16)}
    for key, name in zip(kw, NAMES, strict=True):
        w = jax.random.normal(key, SHAPES[name], jnp.float32) * SHAPES[name][1] ** -0.5
        drawn[name] = (w * {"w_gate": 1.0, "w_up": bump(kh, FF, 4.0), "w_down": layers}[name]).astype(jnp.bfloat16)
    for key, name in zip(km, NAMES, strict=True):
        drawn[f"m_{name}"] = 0.1 * jax.random.normal(key, SHAPES[name], jnp.float32)
    for key, name in zip(kv, NAMES, strict=True):
        drawn[f"v_{name}"] = jax.random.uniform(key, SHAPES[name], jnp.float32, 0.005, 0.015)
    return drawn


def matmul(a, w):
    return jnp.dot(a, w, preferred_element_type=jnp.float32).astype(jnp.bfloat16)


def normed(h):
    wide = h.astype(jnp.float32)
    scale = lax.rsqrt(jnp.mean(wide**2, -1, keepdims=True) + 1e-6)
    return (wide * scale).astype(jnp.bfloat16)


def layer(h, w):
    a = normed(h)
    gate = jnp.dot(a, w["w_gate"], preferred_element_type=jnp.float32)
    up = jnp.dot(a, w["w_up"], preferred_element_type=jnp.float32)
    return h + matmul((jax.nn.silu(gate) * up).astype(jnp.bfloat16), w["w_down"])


def adamw(w, m, v, g):
    m = 0.9 * m + 0.1 * g
    v = 0.95 * v + 0.05 * g * g
    step = m * lax.rsqrt(v + 1e-8) + 0.1 * w
    return (w - 0.02 * step).astype(jnp.bfloat16), m, v


def clipped(gradients, sum_of_squares, count):
    factor = jnp.minimum(1.0, 0.5 * lax.rsqrt(sum_of_squares / count + 1e-30))
    return [g * factor for g in gradients]


def stack(weights, h):
    return lax.scan(lambda h, w: (layer(h, w), None), h, weights)[0]


def reference(x, dy, w_gate, w_up, w_down, m_w_gate, m_w_up, m_w_down, v_w_gate, v_w_up, v_w_down):
    weights = dict(zip(NAMES, (w_gate, w_up, w_down), strict=True))

    def take(so_far, sequence):
        h, by_y = sequence
        _, back = jax.vjp(lambda w: stack(w, h), weights)
        return jax.tree.map(lambda total, term: total + term.astype(jnp.float32), so_far, back(by_y)[0]), None

    none_yet = {name: jnp.zeros(w.shape, jnp.float32) for name, w in weights.items()}
    by_weights, _ = lax.scan(take, none_yet, (x, dy))
    gradients = [by_weights[name].astype(jnp.bfloat16).astype(jnp.float32) for name in NAMES]
    gradients = clipped(gradients, sum(jnp.sum(g * g) for g in gradients), sum(g.size for g in gradients))
    new = [
        adamw(w.astype(jnp.float32), m, v, g)
        for w, m, v, g in zip((w_gate, w_up, w_down), (m_w_gate, m_w_up, m_w_down), (v_w_gate, v_w_up, v_w_down), gradients, strict=True)
    ]
    return tuple(one[which] for which in range(3) for one in new)
```

```python
import functools

import jax
import jax.numpy as jnp
from jax import lax
from jax.experimental import pallas as pl
from jax.experimental.pallas import tpu as pltpu
from jax.sharding import PartitionSpec as P

F32, BF16 = jnp.float32, jnp.bfloat16
MESH = pl.DeviceIdType.MESH
VMEM, DMA = pltpu.VMEM, pltpu.SemaphoreType.DMA
ANY = pl.BlockSpec(memory_space=pl.ANY)
LIMIT = 63 * 1024 * 1024
CHUNK = 1024
ROWS = 1024


def dot(a, b):
    return jnp.dot(a, b, preferred_element_type=F32)


def dot_t(a, b):
    return lax.dot_general(a, b, (((1,), (1,)), ((), ())), preferred_element_type=F32)


def sigmoid(x):
    return 1.0 / (1.0 + jnp.exp(-x))


def scale_of(wide):
    return lax.rsqrt(jnp.mean(wide * wide, -1, keepdims=True) + 1e-6)


def rows(t, n=ROWS):
    return pl.ds(pl.multiple_of(t * n, n), n)


def weight_copies(layer, c, slot, hbm, buf, sem):
    wg, wu, wd = hbm
    cols = rows(c, CHUNK)
    return [
        pltpu.make_async_copy(wg.at[layer, :, cols], buf[0].at[slot], sem.at[slot, 0]),
        pltpu.make_async_copy(wu.at[layer, :, cols], buf[1].at[slot], sem.at[slot, 1]),
        pltpu.make_async_copy(wd.at[layer, cols, :], buf[2].at[slot], sem.at[slot, 2]),
    ]


def start(copies):
    for c in copies:
        c.start()


def wait(copies):
    for c in copies:
        c.wait()


SMALL = 512


def forward_kernel(x_hbm, wg, wu, wd, h_hbm, gate_hbm, up_hbm, x, a, acc, bg, bu, bd, gs, us, sem, wsem, osem):
    tokens, d = x.shape
    chunks = wg.shape[2] // CHUNK
    blocks = tokens // SMALL
    hbm, buf = (wg, wu, wd), (bg, bu, bd)
    load = pltpu.make_async_copy(x_hbm, x, sem)
    load.start()
    start(weight_copies(0, 0, 0, hbm, buf, wsem))
    load.wait()

    def norm(t, _):
        r = rows(t, SMALL)
        wide = x[r, :].astype(F32)
        a[r, :] = (wide * scale_of(wide)).astype(BF16)
        acc[r, :] = jnp.zeros((SMALL, d), F32)
        return 0

    lax.fori_loop(0, blocks, norm, 0)

    def saves(c, t, slot):
        r = rows(t, SMALL)
        return [
            pltpu.make_async_copy(gs.at[slot], gate_hbm.at[c, r, :], osem.at[slot, 0]),
            pltpu.make_async_copy(us.at[slot], up_hbm.at[c, r, :], osem.at[slot, 1]),
        ]

    def chunk(c, _):
        slot = lax.rem(c, 2)
        wait(weight_copies(0, c, slot, hbm, buf, wsem))

        @pl.when(c + 1 < chunks)
        def _():
            start(weight_copies(0, c + 1, 1 - slot, hbm, buf, wsem))

        def block(t, _):
            s = lax.rem(t, 2)
            r = rows(t, SMALL)

            @pl.when(c * blocks + t >= 2)
            def _():
                wait(saves(c, t, s))

            gate = dot(a[r, :], bg[slot])
            up = dot(a[r, :], bu[slot])
            gs[s] = gate
            us[s] = up
            start(saves(c, t, s))
            hidden = (gate * sigmoid(gate) * up).astype(BF16)
            acc[r, :] += dot(hidden, bd[slot])
            return 0

        lax.fori_loop(0, blocks, block, 0)
        return 0

    lax.fori_loop(0, chunks, chunk, 0)

    def finish(t, _):
        r = rows(t, SMALL)
        x[r, :] = (x[r, :].astype(F32) + acc[r, :].astype(BF16).astype(F32)).astype(BF16)
        return 0

    lax.fori_loop(0, blocks, finish, 0)
    store = pltpu.make_async_copy(x, h_hbm, sem)
    store.start()
    wait(saves(chunks - 1, blocks - 2, 0))
    wait(saves(chunks - 1, blocks - 1, 1))
    store.wait()


def forward(x, weights):
    tokens, d = x.shape
    ff = weights[0].shape[2]
    assert (tokens // SMALL) % 2 == 0
    flops = 6 * tokens * d * ff
    return pl.pallas_call(
        forward_kernel,
        name="forward",
        in_specs=[ANY] * 4,
        out_specs=[ANY] * 3,
        out_shape=[
            jax.ShapeDtypeStruct((tokens, d), BF16),
            jax.ShapeDtypeStruct((ff // CHUNK, tokens, CHUNK), F32),
            jax.ShapeDtypeStruct((ff // CHUNK, tokens, CHUNK), F32),
        ],
        scratch_shapes=[
            VMEM((tokens, d), BF16),
            VMEM((tokens, d), BF16),
            VMEM((tokens, d), F32),
            VMEM((2, d, CHUNK), BF16),
            VMEM((2, d, CHUNK), BF16),
            VMEM((2, CHUNK, d), BF16),
            VMEM((2, SMALL, CHUNK), F32),
            VMEM((2, SMALL, CHUNK), F32),
            DMA,
            DMA((2, 3)),
            DMA((2, 2)),
        ],
        cost_estimate=pl.CostEstimate(flops=flops, bytes_accessed=8 * tokens * ff, transcendentals=tokens * ff),
        compiler_params=pltpu.CompilerParams(vmem_limit_bytes=LIMIT),
    )(x, *weights)


def backward_kernel(layer, *refs):
    last = layer == 1
    take = iter(refs)
    h_hbm, dy_hbm, wg, wu, wd = (next(take) for _ in range(5))
    if not last:
        gate_hbm, up_hbm = next(take), next(take)
    outs = [next(take) for _ in range(3)]
    if last:
        dh_hbm = next(take)
    h, a, at, dy, dyt, bg, bu, bd, hid, dg, du, sg, su, sd = (next(take) for _ in range(14))
    if last:
        accg, accu = next(take), next(take)
        gs = us = None
    else:
        gs, us, gsem = next(take), next(take), next(take)
    sem, wsem, osem = (next(take) for _ in range(3))
    tokens, d = h.shape
    chunks = wg.shape[2] // CHUNK
    hbm, buf = (wg, wu, wd), (bg, bu, bd)
    staged = (sg, su, sd)
    loads = [pltpu.make_async_copy(h_hbm, h, sem.at[0]), pltpu.make_async_copy(dy_hbm, dy, sem.at[1])]
    start(loads)
    start(weight_copies(layer, 0, 0, hbm, buf, wsem))
    n = SMALL
    blocks = tokens // n

    def reads(c, t, slot):
        r = rows(t, n)
        return [
            pltpu.make_async_copy(gate_hbm.at[c, r, :], gs.at[slot], gsem.at[slot, 0]),
            pltpu.make_async_copy(up_hbm.at[c, r, :], us.at[slot], gsem.at[slot, 1]),
        ]

    if not last:
        start(reads(0, 0, 0))
    wait(loads)

    for t in range(tokens // 256):
        r = pl.ds(t * 256, 256)
        wide = h[r, :].astype(F32)
        normal = wide * scale_of(wide)
        a[r, :] = normal.astype(BF16)
        at[:, r] = normal.T.astype(BF16)
        dyt[:, r] = dy[r, :].astype(F32).T.astype(BF16)
    if last:
        accg[...] = jnp.zeros_like(accg)
        accu[...] = jnp.zeros_like(accu)

    def stores(c, slot):
        return [pltpu.make_async_copy(s.at[slot], o.at[:, rows(c, CHUNK)], osem.at[slot, i]) for i, (s, o) in enumerate(zip(staged, outs))]

    def chunk(c, _):
        slot = lax.rem(c, 2)
        wait(weight_copies(layer, c, slot, hbm, buf, wsem))

        @pl.when(c + 1 < chunks)
        def _():
            start(weight_copies(layer, c + 1, 1 - slot, hbm, buf, wsem))

        def block(t, _):
            r = rows(t, n)
            dhid = dot_t(dy[r, :], bd[slot]).astype(BF16).astype(F32)
            if last:
                gate = dot(a[r, :], bg[slot])
                up = dot(a[r, :], bu[slot])
            else:
                s = lax.rem(t, 2)
                wait(reads(c, t, s))
                i = c * blocks + t + 1

                @pl.when(i < chunks * blocks)
                def _():
                    start(reads(i // blocks, lax.rem(i, blocks), 1 - s))

                gate, up = gs[s], us[s]
            sig = sigmoid(gate)
            silu = gate * sig
            hid[r, :] = (silu * up).astype(BF16)
            du_t = (dhid * silu).astype(BF16)
            dg_t = (dhid * up * (sig + silu * (1.0 - sig))).astype(BF16)
            du[r, :] = du_t
            dg[r, :] = dg_t
            if last:
                accg[r, :] += dot_t(dg_t, bg[slot])
                accu[r, :] += dot_t(du_t, bu[slot])
            return 0

        lax.fori_loop(0, blocks, block, 0)

        @pl.when(c >= 2)
        def _():
            wait(stores(c - 2, slot))

        sg[slot] = dot(at[...], dg[...]).astype(BF16)
        su[slot] = dot(at[...], du[...]).astype(BF16)
        sd[slot] = dot(dyt[...], hid[...]).astype(BF16)
        start(stores(c, slot))
        return 0

    lax.fori_loop(0, chunks, chunk, 0)

    if last:

        def finish(t, _):
            r = rows(t, 256)
            da = (accg[r, :].astype(BF16).astype(F32) + accu[r, :].astype(BF16).astype(F32)).astype(BF16).astype(F32)
            wide = h[r, :].astype(F32)
            scale = scale_of(wide)
            along = jnp.sum(da * wide, -1, keepdims=True)
            dh = (da * scale - wide * (scale * scale * scale * along * (1.0 / d))).astype(BF16)
            a[r, :] = (dy[r, :].astype(F32) + dh.astype(F32)).astype(BF16)
            return 0

        lax.fori_loop(0, tokens // 256, finish, 0)
        back = pltpu.make_async_copy(a, dh_hbm, sem.at[0])
        back.start()
        back.wait()
    wait(stores(chunks - 2, 0))
    wait(stores(chunks - 1, 1))


def backward(layer, h, dy, weights, saved=()):
    tokens, d = h.shape
    ff = weights[0].shape[2]
    last = layer == 1
    matmuls = 8 if last else 4
    out = [jax.ShapeDtypeStruct((d, ff), BF16)] * 3
    scratch = [VMEM((tokens, d), BF16), VMEM((tokens, d), BF16), VMEM((d, tokens), BF16), VMEM((tokens, d), BF16), VMEM((d, tokens), BF16)]
    scratch += [VMEM((2, d, CHUNK), BF16), VMEM((2, d, CHUNK), BF16), VMEM((2, CHUNK, d), BF16)]
    scratch += [VMEM((tokens, CHUNK), BF16)] * 3 + [VMEM((2, d, CHUNK), BF16)] * 3
    if last:
        out.append(jax.ShapeDtypeStruct((tokens, d), BF16))
        scratch += [VMEM((tokens, d), F32)] * 2
    else:
        scratch += [VMEM((2, SMALL, CHUNK), F32)] * 2 + [DMA((2, 2))]
    scratch += [DMA((2,)), DMA((2, 3)), DMA((2, 3))]
    return pl.pallas_call(
        functools.partial(backward_kernel, layer),
        name=f"backward{layer}",
        in_specs=[ANY] * (5 + len(saved)),
        out_specs=[ANY] * len(out),
        out_shape=out,
        scratch_shapes=scratch,
        cost_estimate=pl.CostEstimate(flops=2 * matmuls * tokens * d * ff, bytes_accessed=8 * tokens * ff, transcendentals=tokens * ff),
        compiler_params=pltpu.CompilerParams(vmem_limit_bytes=LIMIT),
    )(h, dy, *weights, *saved)


def total_kernel(n, part_ref, out_ref, slots, ssem, rsem):
    me = lax.axis_index("dp")
    barrier = pltpu.get_barrier_semaphore()
    for k in range(1, n):
        pl.semaphore_signal(barrier, inc=1, device_id={"dp": lax.bitwise_xor(me, k)}, device_id_type=MESH)
    pl.semaphore_wait(barrier, n - 1)
    copies = [
        pltpu.make_async_remote_copy(part_ref, slots.at[k], ssem.at[k], rsem.at[k], device_id={"dp": lax.bitwise_xor(me, k)}, device_id_type=MESH)
        for k in range(1, n)
    ]
    start(copies)
    wait(copies)
    slots[0] = part_ref[...]
    out_ref[...] = functools.reduce(lambda a, b: a + b, [slots[lax.bitwise_xor(me, k)] for k in range(n)])


def total(part, n):
    return pl.pallas_call(
        functools.partial(total_kernel, n),
        name="total",
        in_specs=[pl.BlockSpec(memory_space=VMEM)],
        out_specs=pl.BlockSpec(memory_space=VMEM),
        out_shape=jax.ShapeDtypeStruct((8, 128), F32),
        scratch_shapes=[VMEM((n, 8, 128), F32), DMA((n,)), DMA((n,))],
        compiler_params=pltpu.CompilerParams(collective_id=0, has_side_effects=True),
    )(jnp.broadcast_to(part, (8, 128)))[0, 0]


def assemble(blocks, name):
    layers, n = len(blocks), len(blocks[0])
    flat = [b for of_layer in blocks for b in of_layer]
    height, width = flat[0].shape
    slots = 8

    def kernel(*refs):
        ins, out, buf, isem, osem = refs[: len(flat)], *refs[len(flat) :]
        me = lax.axis_index("dp")

        def bring(i):
            return pltpu.make_async_copy(ins[i], buf.at[i % slots], isem.at[i % slots])

        def put(i):
            layer, k = divmod(i, n)
            return pltpu.make_async_copy(buf.at[i % slots], out.at[layer, rows(lax.bitwise_xor(me, k), height), :], osem.at[i % slots])

        half = slots // 2
        for i in range(half):
            bring(i).start()
        for i in range(len(flat)):
            bring(i).wait()
            put(i).start()
            if i + half < len(flat):
                if i + half >= slots:
                    put(i + half - slots).wait()
                bring(i + half).start()
        for i in range(len(flat) - slots, len(flat)):
            put(i).wait()

    return pl.pallas_call(
        kernel,
        name=name,
        in_specs=[ANY] * len(flat),
        out_specs=ANY,
        out_shape=jax.ShapeDtypeStruct((layers, n * height, width), BF16),
        scratch_shapes=[VMEM((slots, height, width), BF16), DMA((slots,)), DMA((slots,))],
        cost_estimate=pl.CostEstimate(flops=10**7, bytes_accessed=4 * len(flat) * height * width, transcendentals=0),
        compiler_params=pltpu.CompilerParams(vmem_limit_bytes=20 * 1024 * 1024),
    )(*flat)


def from_partner(a, k, n=8):
    return lax.ppermute(a, "dp", [(i, i ^ k) for i in range(n)])


def gathered(w):
    half = w.shape[0] // 2
    by_x, by_y = from_partner(w, 4), from_partner(w, 2)
    far = jnp.concatenate([from_partner(by_x[:half], 2), from_partner(by_y[half:], 4)], 0)
    blocks = []
    for b in (w, by_y, by_x, far):
        blocks += [b, from_partner(b, 1)]
    return blocks


def solution(mesh):
    n = mesh.shape["dp"]

    def step(x, dy, *arrays):
        weights, moments, seconds = (arrays[i : i + 3] for i in (0, 3, 6))
        x, dy = x[0], dy[0]
        me = lax.axis_index("dp")
        h, gate, up = forward(x, weights)
        *grads1, dh = backward(1, h, dy, weights)
        grads0 = backward(0, x, dh, weights, (gate, up))
        mine = []
        for i in range(3):
            each = [lax.psum_scatter(g[i], "dp", scatter_dimension=1 if i == 2 else 0, tiled=True) for g in (grads0, grads1)]
            if i == 2:
                each = [g.T for g in each]
            mine.append(jnp.stack(each).astype(F32))
        squares = total(sum(jnp.sum(g * g) for g in mine), n)
        factor = jnp.minimum(1.0, 0.5 * lax.rsqrt(squares / sum(g.size * n for g in mine) + 1e-30))
        new = []
        for w, m, v, g in zip(weights, moments, seconds, mine, strict=True):
            w = lax.dynamic_slice_in_dim(w, me * m.shape[1], m.shape[1], 1).astype(F32)
            g = g * factor
            m = 0.9 * m + 0.1 * g
            v = 0.95 * v + 0.05 * g * g
            new.append(((w - 0.02 * (m * lax.rsqrt(v + 1e-8) + 0.1 * w)).astype(BF16), m, v))
        whole = [assemble([gathered(w[layer]) for layer in range(2)], f"assemble{i}") for i, (w, _, _) in enumerate(new)]
        return (*whole, *(m for _, m, _ in new), *(v for _, _, v in new))

    tokens = P(("rep", "dp"), None, None)
    held = P(None, "dp", None)
    own = P("rep", "dp", None)
    return jax.shard_map(
        step,
        mesh=mesh,
        in_specs=(tokens, tokens, *[P()] * 3, *[held] * 6),
        out_specs=(*[P("rep")] * 3, *[own] * 6),
        check_vma=False,
    )
```

```python
import functools

import jax
import jax.numpy as jnp
from jax import lax
from jax.experimental import pallas as pl
from jax.experimental.pallas import tpu as pltpu
from jax.sharding import PartitionSpec as P

F32, BF16 = jnp.float32, jnp.bfloat16
MESH = pl.DeviceIdType.MESH
VMEM, DMA = pltpu.VMEM, pltpu.SemaphoreType.DMA
ANY = pl.BlockSpec(memory_space=pl.ANY)
LIMIT = 63 * 1024 * 1024
CHUNK = 1024
LANES = 128
OWN = 1024


def dot(a, b):
    return jnp.dot(a, b, preferred_element_type=F32)


def dot_t(a, b):
    return lax.dot_general(a, b, (((1,), (1,)), ((), ())), preferred_element_type=F32)


def sigmoid(x):
    return 1.0 / (1.0 + jnp.exp(-x))


def scale_of(wide):
    return lax.rsqrt(jnp.mean(wide * wide, -1, keepdims=True) + 1e-6)


def rows(t, n):
    return pl.ds(pl.multiple_of(t * n, n), n)


def columns(c, position):
    owner = (position & 3) * 2 + (position >> 2)
    return pl.ds(pl.multiple_of(owner * OWN + c * LANES, LANES), LANES)


def weight_copies(layer, c, slot, hbm, buf, sem):
    copies = []
    for position in range(CHUNK // LANES):
        here, there = pl.ds(position * LANES, LANES), columns(c, position)
        for i, (w, b) in enumerate(zip(hbm, buf)):
            if w is None:
                continue
            if i < 2:
                copies.append(pltpu.make_async_copy(w.at[layer, :, there], b.at[slot, :, here], sem.at[slot, i]))
            else:
                copies.append(pltpu.make_async_copy(w.at[layer, there, :], b.at[slot, here, :], sem.at[slot, i]))
    return copies


def weight_waits(layer, slot, hbm, buf, sem):
    waits = []
    for i, (w, b) in enumerate(zip(hbm, buf)):
        if w is not None:
            whole = w.at[layer, :, pl.ds(0, CHUNK)] if i < 2 else w.at[layer, pl.ds(0, CHUNK), :]
            waits.append(pltpu.make_async_copy(whole, b.at[slot], sem.at[slot, i]))
    return waits


def start(copies):
    for c in copies:
        c.start()


def wait(copies):
    for c in copies:
        c.wait()


SMALL = 512


def forward_kernel(x_hbm, wg, wu, wd, h_hbm, gate_hbm, up_hbm, x, a, acc, bg, bu, bd, gs, us, sem, wsem, osem):
    tokens, d = x.shape
    chunks = wg.shape[2] // CHUNK
    blocks = tokens // SMALL
    hbm, buf = (wg, wu, wd), (bg, bu, bd)
    load = pltpu.make_async_copy(x_hbm, x, sem)
    load.start()
    start(weight_copies(0, 0, 0, hbm, buf, wsem))
    load.wait()

    def norm(t, _):
        r = rows(t, SMALL)
        wide = x[r, :].astype(F32)
        a[r, :] = (wide * scale_of(wide)).astype(BF16)
        acc[r, :] = jnp.zeros((SMALL, d), F32)
        return 0

    lax.fori_loop(0, blocks, norm, 0)

    def saves(c, t, slot):
        r = rows(t, SMALL)
        return [
            pltpu.make_async_copy(gs.at[slot], gate_hbm.at[c, r, :], osem.at[slot, 0]),
            pltpu.make_async_copy(us.at[slot], up_hbm.at[c, r, :], osem.at[slot, 1]),
        ]

    def chunk(c, _):
        slot = lax.rem(c, 2)
        wait(weight_waits(0, slot, hbm, buf, wsem))

        @pl.when(c + 1 < chunks)
        def _():
            start(weight_copies(0, c + 1, 1 - slot, hbm, buf, wsem))

        def block(t, _):
            s = lax.rem(t, 2)
            r = rows(t, SMALL)

            @pl.when(c * blocks + t >= 2)
            def _():
                wait(saves(c, t, s))

            gate = dot(a[r, :], bg[slot])
            up = dot(a[r, :], bu[slot])
            gs[s] = gate
            us[s] = up
            start(saves(c, t, s))
            hidden = (gate * sigmoid(gate) * up).astype(BF16)
            acc[r, :] += dot(hidden, bd[slot])
            return 0

        lax.fori_loop(0, blocks, block, 0)
        return 0

    lax.fori_loop(0, chunks, chunk, 0)

    def finish(t, _):
        r = rows(t, SMALL)
        x[r, :] = (x[r, :].astype(F32) + acc[r, :].astype(BF16).astype(F32)).astype(BF16)
        return 0

    lax.fori_loop(0, blocks, finish, 0)
    store = pltpu.make_async_copy(x, h_hbm, sem)
    store.start()
    wait(saves(chunks - 1, blocks - 2, 0))
    wait(saves(chunks - 1, blocks - 1, 1))
    store.wait()


def forward(x, weights):
    tokens, d = x.shape
    ff = weights[0].shape[2]
    assert (tokens // SMALL) % 2 == 0
    flops = 6 * tokens * d * ff
    return pl.pallas_call(
        forward_kernel,
        name="forward",
        in_specs=[ANY] * 4,
        out_specs=[ANY] * 3,
        out_shape=[
            jax.ShapeDtypeStruct((tokens, d), BF16),
            jax.ShapeDtypeStruct((ff // CHUNK, tokens, CHUNK), F32),
            jax.ShapeDtypeStruct((ff // CHUNK, tokens, CHUNK), F32),
        ],
        scratch_shapes=[
            VMEM((tokens, d), BF16),
            VMEM((tokens, d), BF16),
            VMEM((tokens, d), F32),
            VMEM((2, d, CHUNK), BF16),
            VMEM((2, d, CHUNK), BF16),
            VMEM((2, CHUNK, d), BF16),
            VMEM((2, SMALL, CHUNK), F32),
            VMEM((2, SMALL, CHUNK), F32),
            DMA,
            DMA((2, 3)),
            DMA((2, 2)),
        ],
        cost_estimate=pl.CostEstimate(flops=flops, bytes_accessed=8 * tokens * ff, transcendentals=tokens * ff),
        compiler_params=pltpu.CompilerParams(vmem_limit_bytes=LIMIT),
    )(x, *weights)


class Sum:
    SCRATCH = (
        [VMEM((3, 2, 2, 2, 2, 256, LANES), BF16), VMEM((2, 3, 2, 2, 2, 256, LANES), BF16)]
        + [VMEM((2, 3, 2, 2, 256, LANES), BF16), VMEM((3, 3, 2, 2, 256, LANES), BF16), VMEM((2, 3, 2, 2, 256, LANES), F32)]
        + [VMEM((2, 3, 2, 256, LANES), BF16), VMEM((3, 3, 2, 256, LANES), BF16), VMEM((2, 3, 2, 256, LANES), F32)]
        + [VMEM((2, 3, 2, 256, LANES), BF16), VMEM((256, LANES), F32)]
        + [DMA((3,)), DMA((2, 3)), DMA((2, 3, 2)), DMA((3, 3, 2)), DMA((2, 3, 2)), DMA((3, 3, 2)), DMA((2, 3))]
    )

    def __init__(self, chunks, out_hbm, refs):
        self.chunks, self.out_hbm = chunks, out_hbm
        self.terms, self.r1, self.p2, self.r2, self.k2, self.p3, self.r3, self.k3, self.sums, self.squares = refs[:10]
        self.s1_sem, self.r1_sem, self.s2_sem, self.r2_sem, self.s3_sem, self.r3_sem, self.out_sem = refs[10:]
        self.me = lax.axis_index("dp")
        self.core, self.x, self.y = lax.rem(self.me, 2), self.me // 4, lax.rem(self.me // 2, 2)

    def barrier(self):
        sem = pltpu.get_barrier_semaphore()
        for k in (1, 2, 4):
            pl.semaphore_signal(sem, inc=1, device_id={"dp": lax.bitwise_xor(self.me, k)}, device_id_type=MESH)
        pl.semaphore_wait(sem, 3)
        self.squares[...] = jnp.zeros_like(self.squares)

    def to(self, k, src, dst, send, recv):
        return pltpu.make_async_remote_copy(src, dst, send, recv, device_id={"dp": lax.bitwise_xor(self.me, k)}, device_id_type=MESH)

    def first(self, c, i):
        slot = lax.rem(c, 2)
        return self.to(1, self.terms.at[i, 1 - self.core], self.r1.at[slot, i], self.s1_sem.at[i], self.r1_sem.at[slot, i])

    def second(self, c, i, half):
        s, r = lax.rem(c, 2), lax.rem(c, 3)
        return self.to((4, 2)[half], self.p2.at[s, i, half], self.r2.at[r, i, half], self.s2_sem.at[s, i, half], self.r2_sem.at[r, i, half])

    def third(self, c, i, half):
        s, r = lax.rem(c, 2), lax.rem(c, 3)
        return self.to((2, 4)[half], self.p3.at[s, i, half], self.r3.at[r, i, half], self.s3_sem.at[s, i, half], self.r3_sem.at[r, i, half])

    def out(self, c, i):
        slot = lax.rem(c, 2)
        return pltpu.make_async_copy(self.sums.at[slot, i], self.out_hbm.at[c, i], self.out_sem.at[slot, i])

    def put_rows(self, i, part, block):
        for core in range(2):
            for p in range(4):
                for j in range(4):
                    piece = block[(core * 4 + p) * 64 : (core * 4 + p) * 64 + 64, j * LANES : j * LANES + LANES]
                    self.terms[i, core, p // 2, p % 2, part, j * 64 : j * 64 + 64, :] = piece

    def put_columns(self, part, block):
        for p in range(4):
            for half in range(2):
                self.terms[2, part, p // 2, p % 2, half] = block[half * 256 : half * 256 + 256, p * LANES : p * LANES + LANES]

    def on_two(self, c, i):
        self.first(c, i).wait_recv()
        self.first(c, i).wait_send()

        @pl.when(c >= 2)
        def _():
            for half in range(2):
                self.second(c - 2, i, half).wait_send()

        s = lax.rem(c, 2)

        def pair(x, y, half):
            return self.terms[i, self.core, x, y, half].astype(F32) + self.r1[s, i, x, y, half].astype(F32)

        for z in range(2):
            self.p2[s, i, 0, z] = pair(1 - self.x, z, 0).astype(BF16)
            self.p2[s, i, 1, z] = pair(z, 1 - self.y, 1).astype(BF16)
        for half in range(2):
            self.second(c, i, half).start()
        for z in range(2):
            self.k2[s, i, 0, z] = pair(self.x, z, 0)
            self.k2[s, i, 1, z] = pair(z, self.y, 1)

    def on_four(self, c, i):
        for half in range(2):
            self.second(c, i, half).wait_recv()

        @pl.when(c >= 2)
        def _():
            for half in range(2):
                self.third(c - 2, i, half).wait_send()

        s, r = lax.rem(c, 2), lax.rem(c, 3)
        for half, z in ((0, self.y), (1, self.x)):
            self.p3[s, i, half] = (self.k2[s, i, half, 1 - z] + self.r2[r, i, half, 1 - z].astype(F32)).astype(BF16)
        for half in range(2):
            self.third(c, i, half).start()
        for half, z in ((0, self.y), (1, self.x)):
            self.k3[s, i, half] = self.k2[s, i, half, z] + self.r2[r, i, half, z].astype(F32)

    def on_all(self, c, i):
        for half in range(2):
            self.third(c, i, half).wait_recv()

        @pl.when(c >= 2)
        def _():
            self.out(c - 2, i).wait()

        s, r = lax.rem(c, 2), lax.rem(c, 3)
        for half in range(2):
            g = (self.k3[s, i, half] + self.r3[r, i, half].astype(F32)).astype(BF16)
            self.sums[s, i, half] = g
            g = g.astype(F32)
            self.squares[...] += g * g
        self.out(c, i).start()

    def stage(self, c, i):
        for back, work in ((1, self.on_two), (2, self.on_four), (3, self.on_all)):

            @pl.when(jnp.logical_and(c >= back, c < self.chunks + back))
            def _():
                work(c - back, i)

    def finish(self):
        def step(k, _):
            c = self.chunks + k // 3
            self.stage(c, lax.rem(k, 3))
            return 0

        lax.fori_loop(0, 9, step, 0)
        for c in (self.chunks - 2, self.chunks - 1):
            for i in range(3):
                for half in range(2):
                    self.second(c, i, half).wait_send()
                    self.third(c, i, half).wait_send()
                self.out(c, i).wait()


def backward_kernel(layer, *refs):
    last = layer == 1
    take = iter(refs)
    h_hbm, dy_hbm = next(take), next(take)
    if last:
        hbm = [next(take) for _ in range(3)]
    else:
        hbm = [None, None, next(take)]
        gate_hbm, up_hbm = next(take), next(take)
    sums_hbm, squares_out = next(take), next(take)
    if last:
        dh_hbm = next(take)
    a, at, dy, dyt = (next(take) for _ in range(4))
    if last:
        buf = [next(take) for _ in range(3)]
        accg, accu = next(take), next(take)
    else:
        buf = [None, None, next(take)]
        gs, us, gsem = next(take), next(take), next(take)
    hid, dg, du = (next(take) for _ in range(3))
    sem, wsem = next(take), next(take)
    tokens, d = a.shape
    chunks = hbm[2].shape[1] // CHUNK
    total_sum = Sum(chunks, sums_hbm, list(take))
    loads = [pltpu.make_async_copy(h_hbm, a, sem.at[0]), pltpu.make_async_copy(dy_hbm, dy, sem.at[1])]
    start(loads)
    start(weight_copies(layer, 0, 0, hbm, buf, wsem))
    n = SMALL
    blocks = tokens // n

    def reads(c, t, slot):
        r = rows(t, n)
        return [
            pltpu.make_async_copy(gate_hbm.at[c, r, :], gs.at[slot], gsem.at[slot, 0]),
            pltpu.make_async_copy(up_hbm.at[c, r, :], us.at[slot], gsem.at[slot, 1]),
        ]

    if not last:
        start(reads(0, 0, 0))
    total_sum.barrier()
    wait(loads)

    for t in range(tokens // 256):
        r = pl.ds(t * 256, 256)
        wide = a[r, :].astype(F32)
        normal = wide * scale_of(wide)
        if last:
            a[r, :] = normal.astype(BF16)
        turned = normal.T.astype(BF16)
        for owner in range(8):
            position = (owner % 2) * 4 + owner // 2
            at[position * 64 : position * 64 + 64, r] = turned[owner * 64 : owner * 64 + 64, :]
        dyt[:, r] = dy[r, :].astype(F32).T.astype(BF16)
    if last:
        accg[...] = jnp.zeros_like(accg)
        accu[...] = jnp.zeros_like(accu)

    def chunk(c, _):
        slot = lax.rem(c, 2)
        wait(weight_waits(layer, slot, hbm, buf, wsem))

        @pl.when(c + 1 < chunks)
        def _():
            start(weight_copies(layer, c + 1, 1 - slot, hbm, buf, wsem))

        def block(t, _):
            @pl.when(t < 3)
            def _():
                total_sum.stage(c, t)

            r = rows(t, n)
            dhid = dot_t(dy[r, :], buf[2][slot]).astype(BF16).astype(F32)
            if last:
                gate = dot(a[r, :], buf[0][slot])
                up = dot(a[r, :], buf[1][slot])
            else:
                s = lax.rem(t, 2)
                wait(reads(c, t, s))
                i = c * blocks + t + 1

                @pl.when(i < chunks * blocks)
                def _():
                    start(reads(i // blocks, lax.rem(i, blocks), 1 - s))

                gate, up = gs[s], us[s]
            sig = sigmoid(gate)
            silu = gate * sig
            hid[r, :] = (silu * up).astype(BF16)
            du_t = (dhid * silu).astype(BF16)
            dg_t = (dhid * up * (sig + silu * (1.0 - sig))).astype(BF16)
            du[r, :] = du_t
            dg[r, :] = dg_t
            if last:
                accg[r, :] += dot_t(dg_t, buf[0][slot])
                accu[r, :] += dot_t(du_t, buf[1][slot])
            return 0

        lax.fori_loop(0, blocks, block, 0)
        for i, by in ((0, dg), (1, du)):
            for part in range(2):
                total_sum.put_rows(i, part, dot(at[...], by[:, part * 512 : part * 512 + 512]).astype(BF16))
            total_sum.first(c, i).start()
        for part in range(2):
            total_sum.put_columns(part, dot(dyt[...], hid[:, part * 512 : part * 512 + 512]).astype(BF16))
        total_sum.first(c, 2).start()
        return 0

    lax.fori_loop(0, chunks, chunk, 0)

    if last:
        again = pltpu.make_async_copy(h_hbm, a, sem.at[0])
        again.start()
        again.wait()

        def finish(t, _):
            r = rows(t, 256)
            da = (accg[r, :].astype(BF16).astype(F32) + accu[r, :].astype(BF16).astype(F32)).astype(BF16).astype(F32)
            wide = a[r, :].astype(F32)
            scale = scale_of(wide)
            along = jnp.sum(da * wide, -1, keepdims=True)
            dh = (da * scale - wide * (scale * scale * scale * along * (1.0 / d))).astype(BF16)
            a[r, :] = (dy[r, :].astype(F32) + dh.astype(F32)).astype(BF16)
            return 0

        lax.fori_loop(0, tokens // 256, finish, 0)
        back = pltpu.make_async_copy(a, dh_hbm, sem.at[0])
        back.start()
    total_sum.finish()
    squares_out[...] = jnp.sum(total_sum.squares[...].reshape(32, 8, LANES), 0)
    if last:
        back.wait()


def backward(layer, h, dy, weights, saved=()):
    tokens, d = h.shape
    ff = weights[2].shape[1]
    last = layer == 1
    matmuls = 8 if last else 4
    weights = weights if last else weights[2:]
    out = [jax.ShapeDtypeStruct((ff // CHUNK, 3, 2, 256, LANES), BF16), jax.ShapeDtypeStruct((8, LANES), F32)]
    specs = [ANY, pl.BlockSpec(memory_space=VMEM)]
    scratch = [VMEM((tokens, d), BF16), VMEM((d, tokens), BF16), VMEM((tokens, d), BF16), VMEM((d, tokens), BF16)]
    if last:
        out.append(jax.ShapeDtypeStruct((tokens, d), BF16))
        specs.append(ANY)
        scratch += [VMEM((2, d, CHUNK), BF16), VMEM((2, d, CHUNK), BF16), VMEM((2, CHUNK, d), BF16)]
        scratch += [VMEM((tokens, d), F32)] * 2
    else:
        scratch += [VMEM((2, CHUNK, d), BF16)]
        scratch += [VMEM((2, SMALL, CHUNK), F32)] * 2 + [DMA((2, 2))]
    scratch += [VMEM((tokens, CHUNK), BF16)] * 3
    scratch += [DMA((2,)), DMA((2, 3)), *Sum.SCRATCH]
    return pl.pallas_call(
        functools.partial(backward_kernel, layer),
        name=f"backward{layer}",
        in_specs=[ANY] * (2 + len(weights) + len(saved)),
        out_specs=specs,
        out_shape=out,
        scratch_shapes=scratch,
        cost_estimate=pl.CostEstimate(flops=2 * matmuls * tokens * d * ff, bytes_accessed=8 * tokens * ff, transcendentals=tokens * ff),
        compiler_params=pltpu.CompilerParams(vmem_limit_bytes=LIMIT, collective_id=1 + layer, has_side_effects=True),
    )(h, dy, *weights, *saved)


def total_kernel(n, part_ref, out_ref, slots, ssem, rsem):
    me = lax.axis_index("dp")
    barrier = pltpu.get_barrier_semaphore()
    for k in range(1, n):
        pl.semaphore_signal(barrier, inc=1, device_id={"dp": lax.bitwise_xor(me, k)}, device_id_type=MESH)
    pl.semaphore_wait(barrier, n - 1)
    copies = [
        pltpu.make_async_remote_copy(part_ref, slots.at[k], ssem.at[k], rsem.at[k], device_id={"dp": lax.bitwise_xor(me, k)}, device_id_type=MESH)
        for k in range(1, n)
    ]
    start(copies)
    wait(copies)
    slots[0] = part_ref[...]
    out_ref[...] = functools.reduce(lambda a, b: a + b, [slots[lax.bitwise_xor(me, k)] for k in range(n)])


def total(part, n):
    return pl.pallas_call(
        functools.partial(total_kernel, n),
        name="total",
        in_specs=[pl.BlockSpec(memory_space=VMEM)],
        out_specs=pl.BlockSpec(memory_space=VMEM),
        out_shape=jax.ShapeDtypeStruct((8, 128), F32),
        scratch_shapes=[VMEM((n, 8, 128), F32), DMA((n,)), DMA((n,))],
        compiler_params=pltpu.CompilerParams(collective_id=0, has_side_effects=True),
    )(jnp.broadcast_to(part, (8, 128)))[0, 0]


def assemble(blocks, name):
    layers, n = len(blocks), len(blocks[0])
    flat = [b for of_layer in blocks for b in of_layer]
    height, width = flat[0].shape
    slots = 8

    def kernel(*refs):
        ins, out, buf, isem, osem = refs[: len(flat)], *refs[len(flat) :]
        me = lax.axis_index("dp")

        def bring(i):
            return pltpu.make_async_copy(ins[i], buf.at[i % slots], isem.at[i % slots])

        def put(i):
            layer, k = divmod(i, n)
            return pltpu.make_async_copy(buf.at[i % slots], out.at[layer, rows(lax.bitwise_xor(me, k), height), :], osem.at[i % slots])

        half = slots // 2
        for i in range(half):
            bring(i).start()
        for i in range(len(flat)):
            bring(i).wait()
            put(i).start()
            if i + half < len(flat):
                if i + half >= slots:
                    put(i + half - slots).wait()
                bring(i + half).start()
        for i in range(len(flat) - slots, len(flat)):
            put(i).wait()

    return pl.pallas_call(
        kernel,
        name=name,
        in_specs=[ANY] * len(flat),
        out_specs=ANY,
        out_shape=jax.ShapeDtypeStruct((layers, n * height, width), BF16),
        scratch_shapes=[VMEM((slots, height, width), BF16), DMA((slots,)), DMA((slots,))],
        cost_estimate=pl.CostEstimate(flops=10**7, bytes_accessed=4 * len(flat) * height * width, transcendentals=0),
        compiler_params=pltpu.CompilerParams(vmem_limit_bytes=20 * 1024 * 1024),
    )(*flat)


def from_partner(a, k, n=8):
    return lax.ppermute(a, "dp", [(i, i ^ k) for i in range(n)])


def gathered(w):
    half = w.shape[0] // 2
    by_x, by_y = from_partner(w, 4), from_partner(w, 2)
    far = jnp.concatenate([from_partner(by_x[:half], 2), from_partner(by_y[half:], 4)], 0)
    blocks = []
    for b in (w, by_y, by_x, far):
        blocks += [b, from_partner(b, 1)]
    return blocks


def own_blocks(sums):
    layers, chunks = sums.shape[:2]
    blocks = []
    for i in range(2):
        g = sums[:, :, i].reshape(layers, chunks, 2, 2, 2, 64, LANES)
        blocks.append(g.transpose(0, 5, 3, 4, 2, 1, 6).reshape(layers, 64, -1))
    blocks.append(sums[:, :, 2].transpose(0, 1, 4, 2, 3).reshape(layers, chunks * LANES, -1))
    return blocks


def solution(mesh):
    n = mesh.shape["dp"]

    def step(x, dy, *arrays):
        weights, moments, seconds = (arrays[i : i + 3] for i in (0, 3, 6))
        x, dy = x[0], dy[0]
        me = lax.axis_index("dp")
        h, gate, up = forward(x, weights)
        sums1, squares1, dh = backward(1, h, dy, weights)
        sums0, squares0 = backward(0, x, dh, weights, (gate, up))
        squares = total(jnp.sum(squares0 + squares1), n)
        mine = own_blocks(jnp.stack([sums0, sums1]).astype(F32))
        factor = jnp.minimum(1.0, 0.5 * lax.rsqrt(squares / sum(g.size * n for g in mine) + 1e-30))
        new = []
        for w, m, v, g in zip(weights, moments, seconds, mine, strict=True):
            w = lax.dynamic_slice_in_dim(w, me * m.shape[1], m.shape[1], 1).astype(F32)
            g = g * factor
            m = 0.9 * m + 0.1 * g
            v = 0.95 * v + 0.05 * g * g
            new.append(((w - 0.02 * (m * lax.rsqrt(v + 1e-8) + 0.1 * w)).astype(BF16), m, v))
        whole = [assemble([gathered(w[layer]) for layer in range(2)], f"assemble{i}") for i, (w, _, _) in enumerate(new)]
        return (*whole, *(m for _, m, _ in new), *(v for _, _, v in new))

    tokens = P(("rep", "dp"), None, None)
    held = P(None, "dp", None)
    own = P("rep", "dp", None)
    return jax.shard_map(
        step,
        mesh=mesh,
        in_specs=(tokens, tokens, *[P()] * 3, *[held] * 6),
        out_specs=(*[P("rep")] * 3, *[own] * 6),
        check_vma=False,
    )
```

```python
import functools

import jax
import jax.numpy as jnp
from jax import lax
from jax.experimental import pallas as pl
from jax.experimental.pallas import tpu as pltpu
from jax.sharding import PartitionSpec as P

F32, BF16 = jnp.float32, jnp.bfloat16
MESH = pl.DeviceIdType.MESH
VMEM, DMA = pltpu.VMEM, pltpu.SemaphoreType.DMA
ANY = pl.BlockSpec(memory_space=pl.ANY)
LIMIT = 63 * 1024 * 1024
CHUNK = 1024
PART = 512
LANES = 128
OWN = 1024


def dot(a, b):
    return jnp.dot(a, b, preferred_element_type=F32)


def dot_t(a, b):
    return lax.dot_general(a, b, (((1,), (1,)), ((), ())), preferred_element_type=F32)


def sigmoid(x):
    return 1.0 / (1.0 + jnp.exp(-x))


def scale_of(wide):
    return lax.rsqrt(jnp.mean(wide * wide, -1, keepdims=True) + 1e-6)


def rows(t, n):
    return pl.ds(pl.multiple_of(t * n, n), n)


def columns(c, position):
    owner = (position & 3) * 2 + (position >> 2)
    return pl.ds(pl.multiple_of(owner * OWN + c * LANES, LANES), LANES)


def weight_copies(layer, c, slot, hbm, buf, sem, positions=range(8)):
    copies = []
    for i, (w, b) in enumerate(zip(hbm, buf)):
        for k, position in enumerate(positions):
            here, there = pl.ds(k * LANES, LANES), columns(c, position)
            if w is None:
                continue
            if i < 2:
                copies.append(pltpu.make_async_copy(w.at[layer, :, there], b.at[slot, :, here], sem.at[slot, i]))
            else:
                copies.append(pltpu.make_async_copy(w.at[layer, there, :], b.at[slot, here, :], sem.at[slot, i]))
    return copies


def weight_waits(layer, slot, hbm, buf, sem, width=CHUNK):
    waits = []
    for i, (w, b) in enumerate(zip(hbm, buf)):
        if w is not None:
            whole = w.at[layer, :, pl.ds(0, width)] if i < 2 else w.at[layer, pl.ds(0, width), :]
            waits.append(pltpu.make_async_copy(whole, b.at[slot], sem.at[slot, i]))
    return waits


def start(copies):
    for c in copies:
        c.start()


def wait(copies):
    for c in copies:
        c.wait()


SMALL = 512


def forward_kernel(x_hbm, wg, wu, wd, h_hbm, gate_hbm, up_hbm, x, a, acc, bg, bu, bd, gs, us, sem, wsem, osem):
    tokens, d = x.shape
    chunks = wg.shape[2] // CHUNK
    blocks = tokens // SMALL
    hbm, buf = (wg, wu, wd), (bg, bu, bd)
    load = pltpu.make_async_copy(x_hbm, x, sem)
    load.start()
    start(weight_copies(0, 0, 0, hbm, buf, wsem))
    load.wait()

    def norm(t, _):
        r = rows(t, SMALL)
        wide = x[r, :].astype(F32)
        a[r, :] = (wide * scale_of(wide)).astype(BF16)
        acc[r, :] = jnp.zeros((SMALL, d), F32)
        return 0

    lax.fori_loop(0, blocks, norm, 0)

    def saves(c, t, slot):
        r = rows(t, SMALL)
        return [
            pltpu.make_async_copy(b.at[slot, :, pl.ds(part * PART, PART)], o.at[c * 2 + part, r, :], osem.at[slot, i, part])
            for i, (b, o) in enumerate(((gs, gate_hbm), (us, up_hbm)))
            for part in range(2)
        ]

    def chunk(c, _):
        slot = lax.rem(c, 2)
        wait(weight_waits(0, slot, hbm, buf, wsem))

        @pl.when(c + 1 < chunks)
        def _():
            start(weight_copies(0, c + 1, 1 - slot, hbm, buf, wsem))

        def block(t, _):
            s = lax.rem(t, 2)
            r = rows(t, SMALL)

            @pl.when(c * blocks + t >= 2)
            def _():
                wait(saves(c, t, s))

            gate = dot(a[r, :], bg[slot])
            up = dot(a[r, :], bu[slot])
            gs[s] = gate
            us[s] = up
            start(saves(c, t, s))
            hidden = (gate * sigmoid(gate) * up).astype(BF16)
            acc[r, :] += dot(hidden, bd[slot])
            return 0

        lax.fori_loop(0, blocks, block, 0)
        return 0

    lax.fori_loop(0, chunks, chunk, 0)

    def finish(t, _):
        r = rows(t, SMALL)
        x[r, :] = (x[r, :].astype(F32) + acc[r, :].astype(BF16).astype(F32)).astype(BF16)
        return 0

    lax.fori_loop(0, blocks, finish, 0)
    store = pltpu.make_async_copy(x, h_hbm, sem)
    store.start()
    wait(saves(chunks - 1, blocks - 2, 0))
    wait(saves(chunks - 1, blocks - 1, 1))
    store.wait()


def forward(x, weights):
    tokens, d = x.shape
    ff = weights[0].shape[2]
    assert (tokens // SMALL) % 2 == 0
    flops = 6 * tokens * d * ff
    return pl.pallas_call(
        forward_kernel,
        name="forward",
        in_specs=[ANY] * 4,
        out_specs=[ANY] * 3,
        out_shape=[
            jax.ShapeDtypeStruct((tokens, d), BF16),
            jax.ShapeDtypeStruct((ff // PART, tokens, PART), F32),
            jax.ShapeDtypeStruct((ff // PART, tokens, PART), F32),
        ],
        scratch_shapes=[
            VMEM((tokens, d), BF16),
            VMEM((tokens, d), BF16),
            VMEM((tokens, d), F32),
            VMEM((2, d, CHUNK), BF16),
            VMEM((2, d, CHUNK), BF16),
            VMEM((2, CHUNK, d), BF16),
            VMEM((2, SMALL, CHUNK), F32),
            VMEM((2, SMALL, CHUNK), F32),
            DMA,
            DMA((2, 3)),
            DMA((2, 2, 2)),
        ],
        cost_estimate=pl.CostEstimate(flops=flops, bytes_accessed=8 * tokens * ff, transcendentals=tokens * ff),
        compiler_params=pltpu.CompilerParams(vmem_limit_bytes=LIMIT),
    )(x, *weights)


QUARTER = 192


class Sum:
    SCRATCH = (
        [VMEM((2, 4, 2, 2, 2, 2, QUARTER, LANES), BF16), VMEM((2, 4, 2, 2, 2, QUARTER, LANES), BF16)]
        + [VMEM((2, 4, 2, 2, QUARTER, LANES), BF16), VMEM((2, 4, 2, 2, QUARTER, LANES), BF16), VMEM((2, 4, 2, 2, QUARTER, LANES), F32)]
        + [VMEM((2, 4, 2, QUARTER, LANES), BF16), VMEM((2, 4, 2, QUARTER, LANES), BF16), VMEM((2, 4, 2, QUARTER, LANES), F32)]
        + [VMEM((2, 4, 2, QUARTER, LANES), BF16), VMEM((QUARTER, LANES), F32), VMEM((8, 8, LANES), F32)]
        + [DMA((4,)), DMA((2, 4)), DMA((2, 4, 2)), DMA((2, 4, 2)), DMA((2, 4, 2)), DMA((2, 4, 2)), DMA((2, 4)), DMA((8,)), DMA((8,))]
    )

    def __init__(self, chunks, out_hbm, refs):
        self.chunks, self.out_hbm = chunks, out_hbm
        self.terms, self.r1, self.p2, self.r2, self.k2, self.p3, self.r3, self.k3, self.sums, self.squares, self.parts = refs[:11]
        self.s1_sem, self.r1_sem, self.s2_sem, self.r2_sem, self.s3_sem, self.r3_sem, self.out_sem, self.s4_sem, self.r4_sem = refs[11:]
        self.me = lax.axis_index("dp")
        self.core, self.x, self.y = lax.rem(self.me, 2), self.me // 4, lax.rem(self.me // 2, 2)

    def barrier(self):
        sem = pltpu.get_barrier_semaphore()
        for k in range(1, 8):
            pl.semaphore_signal(sem, inc=1, device_id={"dp": lax.bitwise_xor(self.me, k)}, device_id_type=MESH)
        pl.semaphore_wait(sem, 7)
        self.squares[...] = jnp.zeros_like(self.squares)

    def to(self, k, src, dst, send, recv):
        return pltpu.make_async_remote_copy(src, dst, send, recv, device_id={"dp": lax.bitwise_xor(self.me, k)}, device_id_type=MESH)

    def first(self, c, q):
        slot = lax.rem(c, 2)
        return self.to(1, self.terms.at[slot, q, 1 - self.core], self.r1.at[slot, q], self.s1_sem.at[q], self.r1_sem.at[slot, q])

    def second(self, c, q, half):
        s = lax.rem(c, 2)
        return self.to((4, 2)[half], self.p2.at[s, q, half], self.r2.at[s, q, half], self.s2_sem.at[s, q, half], self.r2_sem.at[s, q, half])

    def third(self, c, q, half):
        s = lax.rem(c, 2)
        return self.to((2, 4)[half], self.p3.at[s, q, half], self.r3.at[s, q, half], self.s3_sem.at[s, q, half], self.r3_sem.at[s, q, half])

    def out(self, c, q):
        s = lax.rem(c, 2)
        return pltpu.make_async_copy(self.sums.at[s, q], self.out_hbm.at[c, :, rows(q, QUARTER), :], self.out_sem.at[s, q])

    def put_rows(self, slot, i, part, block):
        for j in range(4):
            at = i * 4 + j
            q, r = at // 3, rows(lax.rem(at, 3), 64)
            for core in range(2):
                for p in range(4):
                    piece = block[(core * 4 + p) * 64 : (core * 4 + p) * 64 + 64, j * LANES : j * LANES + LANES]
                    self.terms[slot, q, core, p // 2, p % 2, part, r, :] = piece

    def put_columns(self, slot, part, pair, block):
        for k in range(2):
            for half in range(2):
                piece = block[half * 256 : half * 256 + 256, k * LANES : k * LANES + LANES]
                self.terms[slot, 2, part, pair, k, half, 128:192, :] = piece[:64]
                self.terms[slot, 3, part, pair, k, half] = piece[64:]

    def wait_for_two(self, c, q):
        self.first(c, q).wait_recv()
        self.first(c, q).wait_send()

        @pl.when(c >= 2)
        def _():
            for half in range(2):
                self.second(c - 2, q, half).wait_send()

    def wait_for_four(self, c, q):
        for half in range(2):
            self.second(c, q, half).wait_recv()

        @pl.when(c >= 2)
        def _():
            for half in range(2):
                self.third(c - 2, q, half).wait_send()

    def wait_for_all(self, c, q):
        for half in range(2):
            self.third(c, q, half).wait_recv()

        @pl.when(c >= 2)
        def _():
            self.out(c - 2, q).wait()

    def add_two(self, s, q):
        def pair(x, y, half):
            return self.terms[s, q, self.core, x, y, half].astype(F32) + self.r1[s, q, x, y, half].astype(F32)

        for z in range(2):
            self.p2[s, q, 0, z] = pair(1 - self.x, z, 0).astype(BF16)
            self.p2[s, q, 1, z] = pair(z, 1 - self.y, 1).astype(BF16)
            self.k2[s, q, 0, z] = pair(self.x, z, 0)
            self.k2[s, q, 1, z] = pair(z, self.y, 1)

    def add_four(self, s, q):
        for half, z in ((0, self.y), (1, self.x)):
            self.p3[s, q, half] = (self.k2[s, q, half, 1 - z] + self.r2[s, q, half, 1 - z].astype(F32)).astype(BF16)
            self.k3[s, q, half] = self.k2[s, q, half, z] + self.r2[s, q, half, z].astype(F32)

    def add_all(self, s, q, live=None):
        for half in range(2):
            g = (self.k3[s, q, half] + self.r3[s, q, half].astype(F32)).astype(BF16)
            self.sums[s, q, half] = g
            g = g.astype(F32)
            square = g * g
            if live is not None:
                square = jnp.where(live, square, 0.0)
            self.squares[...] += square

    def send_two(self, c, q):
        for half in range(2):
            self.second(c, q, half).start()

    def send_four(self, c, q):
        for half in range(2):
            self.third(c, q, half).start()

    def before(self, c, q):
        for back, work in ((1, self.wait_for_two), (2, self.wait_for_four), (3, self.wait_for_all)):

            @pl.when(c >= back)
            def _():
                work(c - back, q)

    def add(self, c, q, start=0, start_four=0):
        self.add_two(lax.rem(c + 3 + start, 2), q)
        self.add_four(lax.rem(c + 2 + start_four, 2), q)
        self.add_all(lax.rem(c + 3, 2), q, c >= 3)

    def after(self, c, q):
        for back, work in ((1, self.send_two), (2, self.send_four)):

            @pl.when(c >= back)
            def _():
                work(c - back, q)

        @pl.when(c >= 3)
        def _():
            self.out(c - 3, q).start()

    def finish(self):
        n = self.chunks
        for step in range(3):

            def quarter(q, _):
                works = [(self.wait_for_all, self.add_all, lambda c, q: self.out(c, q).start())]
                works = [(self.wait_for_two, self.add_two, self.send_two), (self.wait_for_four, self.add_four, self.send_four), *works][step:]
                for stage in range(3):
                    for k, work in enumerate(works):
                        c = n - 1 - k
                        work[stage](*((c % 2, q) if stage == 1 else (c, q)))
                return 0

            lax.fori_loop(0, 4, quarter, 0)

    def drain(self):
        n = self.chunks

        def quarter(q, _):
            for c in (n - 2, n - 1):
                for half in range(2):
                    self.second(c, q, half).wait_send()
                    self.third(c, q, half).wait_send()
                self.out(c, q).wait()
            return 0

        lax.fori_loop(0, 4, quarter, 0)

    def total(self):
        self.parts[0] = functools.reduce(lambda a, b: a + b, [self.squares[i * 8 : i * 8 + 8, :] for i in range(QUARTER // 8)])
        copies = [self.to(k, self.parts.at[0], self.parts.at[k], self.s4_sem.at[k], self.r4_sem.at[k]) for k in range(1, 8)]
        start(copies)
        wait(copies)
        return jnp.sum(functools.reduce(lambda a, b: a + b, [self.parts[lax.bitwise_xor(self.me, k)] for k in range(8)]))


BLOCK = 1024


def backward_kernel(x_hbm, h_hbm, dy_hbm, wg, wu, wd, gate_hbm, up_hbm, sums_hbm, factor_out, *refs):
    a, at, dy, dyt, bg, bu, bd, even, odd, gu, acc = refs[:11]
    sem, wsem, gsem = refs[11:14]
    tokens, d = a.shape
    chunks = wd.shape[1] // CHUNK
    sums = Sum(2 * chunks, sums_hbm, refs[14:])
    second = ((wg, wu, wd), (bg, bu, bd))
    first = ((None, None, wd), (None, None, bd))
    blocks = tokens // BLOCK

    def turn():
        def block(t, _):
            r = rows(t, 256)
            wide = a[r, :].astype(F32)
            normal = wide * scale_of(wide)
            a[r, :] = normal.astype(BF16)
            turned = normal.T.astype(BF16)
            for owner in range(8):
                position = (owner % 2) * 4 + owner // 2
                at[position * 64 : position * 64 + 64, r] = turned[owner * 64 : owner * 64 + 64, :]
            dyt[:, r] = dy[r, :].astype(F32).T.astype(BF16)
            return 0

        lax.fori_loop(0, tokens // 256, block, 0)

    def bring(p, part):
        for layer, which, when in ((1, second, p < chunks), (0, first, jnp.logical_and(p >= chunks, p < 2 * chunks))):

            @pl.when(when)
            def _():
                start(weight_copies(layer, lax.rem(p, chunks), part, *which, wsem, range(part * 4, part * 4 + 4)))

    def weight_gradients(chunk, part, b):
        of, slot = (even, odd)[part], lax.rem(chunk + 2, 2)
        sums.put_rows(slot, b, part, dot(at[...], of[b]).astype(BF16))
        sums.put_columns(slot, part, b, dot(dyt[...], of[2, :, rows(b, 256)]).astype(BF16))

    def hidden_gradients(part, r, b):
        of = (even, odd)[part]
        dhid = dot_t(dy[r, :], bd[part]).astype(BF16).astype(F32)
        gate, up = gu[b, 0], gu[b, 1]
        sig = sigmoid(gate)
        silu = gate * sig
        of[2, r, :] = (silu * up).astype(BF16)
        of[1, r, :] = (dhid * silu).astype(BF16)
        of[0, r, :] = (dhid * up * (sig + silu * (1.0 - sig))).astype(BF16)

    def send_terms(c, b):
        @pl.when(b == 0)
        def _():
            sums.first(c, 0).start()

        @pl.when(b == 1)
        def _():
            for q in range(1, 4):
                sums.first(c, q).start()

    def reads(k, b):
        r = rows(b, BLOCK)
        return [pltpu.make_async_copy(s.at[k, r, :], gu.at[b, j], gsem.at[b, j]) for j, s in enumerate((gate_hbm, up_hbm))]

    loads = [pltpu.make_async_copy(h_hbm, a, sem.at[0]), pltpu.make_async_copy(dy_hbm, dy, sem.at[1])]
    start(loads)
    bring(0, 0)
    sums.barrier()
    wait(loads)
    turn()
    acc[...] = jnp.zeros_like(acc)

    def input_gradient(t, _):
        n = 512
        r, k = rows(t, n), rows(lax.rem(t, 2), n)
        da = (acc[0, t // 2, k, :].astype(BF16).astype(F32) + acc[1, t // 2, k, :].astype(BF16).astype(F32)).astype(BF16).astype(F32)
        wide = a[r, :].astype(F32)
        scale = scale_of(wide)
        along = jnp.sum(da * wide, -1, keepdims=True)
        dh = (da * scale - wide * (scale * scale * scale * along * (1.0 / d))).astype(BF16)
        dy[r, :] = (dy[r, :].astype(F32) + dh.astype(F32)).astype(BF16)
        return 0

    load = pltpu.make_async_copy(x_hbm, a, sem.at[0])

    def chunk(p, _):
        is_second = p < chunks
        is_first = jnp.logical_not(is_second)

        @pl.when(p == chunks)
        def _():
            again = pltpu.make_async_copy(h_hbm, a, sem.at[0])
            again.start()
            start(reads(0, 0))
            again.wait()
            lax.fori_loop(0, tokens // 512, input_gradient, 0)
            load.start()

        for part in range(2):
            for layer, which, when in ((1, second, is_second), (0, first, is_first)):

                @pl.when(when)
                def _():
                    wait(weight_waits(layer, part, *which, wsem, PART))

            bring(p + part, 1 - part)
            k = 2 * (p - chunks) + part

            def block(b, _):
                c, q = (p - 1, 2 + b) if part == 0 else (p, b)
                sums.before(c, q)
                r = rows(b, BLOCK)

                @pl.when(is_second)
                def _():
                    gu[b, 0] = dot(a[r, :], bg[part])
                    gu[b, 1] = dot(a[r, :], bu[part])

                @pl.when(jnp.logical_and(is_first, k * blocks + b + 1 < 2 * chunks * blocks))
                def _():
                    start(reads(k + b, 1 - b))

                @pl.when(is_first)
                def _():
                    wait(reads(k, b))

                n = 2 * chunks - 1
                at_0, to_1 = (n - p) // n, (n + 1 - p) // n
                if part == 0:
                    sums.add(c, q, at_0, to_1 - at_0)
                else:
                    sums.add(c, q, 0, at_0)
                hidden_gradients(part, r, b)
                weight_gradients(p - 1 + part, 1 - part, b)

                @pl.when(is_second)
                def _():
                    of = (even, odd)[part]
                    acc[0, b] += dot_t(of[0, r, :], bg[part])
                    acc[1, b] += dot_t(of[1, r, :], bu[part])

                sums.after(c, q)
                if part == 0:

                    @pl.when(p >= 1)
                    def _():
                        send_terms(p - 1, b)

                return 0

            lax.fori_loop(0, blocks, block, 0)
            if part == 0:

                @pl.when(p == chunks)
                def _():
                    load.wait()
                    turn()

        return 0

    lax.fori_loop(0, 2 * chunks, chunk, 0)

    def rest(b, _):
        c = 2 * chunks - 1
        sums.before(c, 2 + b)
        sums.add(c, 2 + b)
        weight_gradients(c, 1, b)
        sums.after(c, 2 + b)
        send_terms(c, b)
        return 0

    lax.fori_loop(0, 2, rest, 0)
    sums.finish()
    count = 6 * d * wd.shape[1]
    factor_out[...] = jnp.minimum(1.0, 0.5 * lax.rsqrt(jnp.full(factor_out.shape, sums.total(), F32) / count + 1e-30))
    sums.drain()


def backward(x, h, dy, weights, gate, up):
    tokens, d = h.shape
    ff = weights[2].shape[1]
    assert PART == d and CHUNK == 2 * d and tokens == 2 * BLOCK and ff == 8 * OWN
    scratch = [VMEM((tokens, d), BF16), VMEM((d, tokens), BF16), VMEM((tokens, d), BF16), VMEM((d, tokens), BF16)]
    scratch += [VMEM((2, d, PART), BF16), VMEM((2, d, PART), BF16), VMEM((2, PART, d), BF16)]
    scratch += [VMEM((3, tokens, PART), BF16), VMEM((3, tokens, PART), BF16), VMEM((2, 2, BLOCK, PART), F32), VMEM((2, 2, BLOCK, d), F32)]
    scratch += [DMA((2,)), DMA((2, 3)), DMA((2, 2)), *Sum.SCRATCH]
    return pl.pallas_call(
        backward_kernel,
        name="backward",
        in_specs=[ANY] * 8,
        out_specs=[ANY, pl.BlockSpec(memory_space=VMEM)],
        out_shape=[jax.ShapeDtypeStruct((2 * ff // CHUNK, 2, 4 * QUARTER, LANES), BF16), jax.ShapeDtypeStruct((8, LANES), F32)],
        scratch_shapes=scratch,
        cost_estimate=pl.CostEstimate(flops=24 * tokens * d * ff, bytes_accessed=16 * tokens * ff, transcendentals=2 * tokens * ff),
        compiler_params=pltpu.CompilerParams(vmem_limit_bytes=67043328, collective_id=1, has_side_effects=True),
    )(x, h, dy, *weights, gate, up)


def assemble(blocks, name):
    layers, n = len(blocks), len(blocks[0])
    flat = [b for of_layer in blocks for b in of_layer]
    height, width = flat[0].shape
    slots = 8

    def kernel(*refs):
        ins, out, buf, isem, osem = refs[: len(flat)], *refs[len(flat) :]
        me = lax.axis_index("dp")

        def bring(i):
            return pltpu.make_async_copy(ins[i], buf.at[i % slots], isem.at[i % slots])

        def put(i):
            layer, k = divmod(i, n)
            return pltpu.make_async_copy(buf.at[i % slots], out.at[layer, rows(lax.bitwise_xor(me, k), height), :], osem.at[i % slots])

        half = slots // 2
        for i in range(half):
            bring(i).start()
        for i in range(len(flat)):
            bring(i).wait()
            put(i).start()
            if i + half < len(flat):
                if i + half >= slots:
                    put(i + half - slots).wait()
                bring(i + half).start()
        for i in range(len(flat) - slots, len(flat)):
            put(i).wait()

    return pl.pallas_call(
        kernel,
        name=name,
        in_specs=[ANY] * len(flat),
        out_specs=ANY,
        out_shape=jax.ShapeDtypeStruct((layers, n * height, width), BF16),
        scratch_shapes=[VMEM((slots, height, width), BF16), DMA((slots,)), DMA((slots,))],
        cost_estimate=pl.CostEstimate(flops=10**7, bytes_accessed=4 * len(flat) * height * width, transcendentals=0),
        compiler_params=pltpu.CompilerParams(vmem_limit_bytes=20 * 1024 * 1024),
    )(*flat)


def from_partner(a, k, n=8):
    return lax.ppermute(a, "dp", [(i, i ^ k) for i in range(n)])


def gathered(w):
    half = w.shape[0] // 2
    by_x, by_y = from_partner(w, 4), from_partner(w, 2)
    far = jnp.concatenate([from_partner(by_x[:half], 2), from_partner(by_y[half:], 4)], 0)
    blocks = []
    for b in (w, by_y, by_x, far):
        blocks += [b, from_partner(b, 1)]
    return blocks


def own_blocks(sums):
    layers, chunks = sums.shape[:2]
    blocks = []
    for i in range(2):
        g = sums[:, :, :, i * 256 : i * 256 + 256].reshape(layers, chunks, 2, 2, 2, 64, LANES)
        blocks.append(g.transpose(0, 5, 3, 4, 2, 1, 6).reshape(layers, 64, -1))
    blocks.append(sums[:, :, :, 512:].transpose(0, 1, 4, 2, 3).reshape(layers, chunks * LANES, -1))
    return blocks


def solution(mesh):
    n = mesh.shape["dp"]

    def step(x, dy, *arrays):
        weights, moments, seconds = (arrays[i : i + 3] for i in (0, 3, 6))
        x, dy = x[0], dy[0]
        me = lax.axis_index("dp")
        h, gate, up = forward(x, weights)
        sums, factor = backward(x, h, dy, weights, gate, up)
        factor = factor[0, 0]
        sums = sums.reshape(2, -1, *sums.shape[1:])[::-1]
        mine = own_blocks(sums.astype(F32))
        new = []
        for w, m, v, g in zip(weights, moments, seconds, mine, strict=True):
            w = lax.dynamic_slice_in_dim(w, me * m.shape[1], m.shape[1], 1).astype(F32)
            g = g * factor
            m = 0.9 * m + 0.1 * g
            v = 0.95 * v + 0.05 * g * g
            new.append(((w - 0.02 * (m * lax.rsqrt(v + 1e-8) + 0.1 * w)).astype(BF16), m, v))
        whole = [assemble([gathered(w[layer]) for layer in range(2)], f"assemble{i}") for i, (w, _, _) in enumerate(new)]
        return (*whole, *(m for _, m, _ in new), *(v for _, _, v in new))

    tokens = P(("rep", "dp"), None, None)
    held = P(None, "dp", None)
    own = P("rep", "dp", None)
    return jax.shard_map(
        step,
        mesh=mesh,
        in_specs=(tokens, tokens, *[P()] * 3, *[held] * 6),
        out_specs=(*[P("rep")] * 3, *[own] * 6),
        check_vma=False,
    )
```
